32 devices in a mesh: dom: 8 (over z, y), slab: 4 (over x, core).
Axes of the slice: x: 2, y: 2, z: 4, core: 2. Of those that a mesh axis runs over, the one named last changes fastest.
Arguments:
- particles: bfloat16 [1536, 32, 1024], P('dom', 'slab'), may hold values from -6 to 6
- refs: bfloat16 [2048, 32, 2048], P('dom', 'slab'), may hold values from -6 to 6
- orient: int32 [1536], P('dom'), may hold values from 0 to 2047, as said below
- shifts: int32 [1536, 8, 2], P('dom'), may hold values from -4 to 4
- tilt: int32 [1536], P('dom'), may hold values from 0 to 15
- wedge: float32 [16, 32, 1024], P(None, 'slab'), may hold values from 0.1 to 1
Outputs:
- new_refs: float32 [2048, 32, 2048], P('dom', 'slab')
- shift_weights: float32 [1536, 8], P('dom')
The draws below stay inside these ranges and needn't reach their ends.
Inputs may be any that keep to these rules, and one draw needn't show every extreme that they name: `orient`: split the particles into aligned blocks of 192 (the rows of one device) and the orientations into ranges of 256. In every block at most 48 particles have orientations in any one range, and in every draw one range holds exactly 48 particles of every block.
All inputs are finite; a program needn't handle non-finite values.
Results may differ from the reference program's by a relative error of at most 0.004.
Values may be sent and summed in bfloat16 or wider, within the bound.
A program may use at most 128 MiB of HBM per device.

```python
import math
import jax
import jax.numpy as jnp
from jax import lax

BOX = 32
ORIENT = 2048
TILTS = 16
NSHIFT = 8
P_DEV = 192
PARTICLES = 1536
ORIENT_DEV = 256
CAP = 48
N_DOM = 8


def draw_orient(key, part):
    pool_size = N_DOM * CAP
    full_owner = jax.random.randint(jax.random.fold_in(key, 7), (), 0, N_DOM)
    pool = jnp.arange(pool_size, dtype=jnp.int32) // CAP
    position = jnp.arange(pool_size, dtype=jnp.int32)

    def one_block(block_key):
        key_one, key_two, key_three, key_four = jax.random.split(block_key, 4)
        ranks = jax.random.permutation(key_one, pool_size).astype(jnp.int32)
        priority = jnp.where(pool == full_owner, position - pool_size, ranks)
        order = jnp.argsort(priority)
        owners = pool[order[:P_DEV]]
        owners = jax.random.permutation(key_two, owners)
        left = jax.random.randint(key_three, (P_DEV,), 0, ORIENT_DEV)
        right = jax.random.randint(key_four, (P_DEV,), 0, ORIENT_DEV)
        local = jnp.maximum(left, right)
        return owners * ORIENT_DEV + local
    keys = jax.random.split(jax.random.fold_in(key, 11), N_DOM)
    return jax.vmap(one_block)(keys).reshape(-1).astype(jnp.int32)


def set_ends(result, key, least, high):
    longest = result.shape.index(max(result.shape))
    spots = []
    for shift in (0, 1):
        where = [jax.random.randint(jax.random.fold_in(key, axis), (), 0, length) for axis, length in enumerate(result.shape)]
        where[longest] = (where[longest] + shift) % result.shape[longest]
        spots.append(tuple(where))
    return result.at[spots[0]].set(least).at[spots[1]].set(high)


def block_scale(key, extent, cuts, smallest, top_value):
    level = 1.0
    for dim, blocks in cuts:
        draws = jax.random.uniform(jax.random.fold_in(jax.random.fold_in(key, 6), dim), (blocks,), jnp.float32, smallest / len(cuts), top_value / len(cuts))
        level = level * jnp.repeat(jnp.exp(draws), extent[dim] // blocks).reshape((-1,) + (1,) * (len(extent) - 1 - dim))
    return level


def scatter_about(stream_key, dims, deviation, limit, pieces=(), kind=jnp.bfloat16):
    entries = jax.random.normal(stream_key, dims, jnp.float32) * deviation
    if len(pieces) > 0:
        entries = block_scale(stream_key, dims, pieces, -0.22, 0.18) * entries
    return jnp.clip(entries, min=-limit, max=limit).astype(kind)


def setup_inputs(seed: int = 0) -> dict:
    key_list = jax.random.split(jax.random.key(seed), 7)
    particles = scatter_about(key_list[0], (PARTICLES, BOX, BOX * BOX), 1.0, 6.0, ((0, 8), (1, 4)))
    refs = scatter_about(key_list[1], (ORIENT, BOX, 2 * BOX * BOX), 1.0, 6.0, ((0, 8), (1, 4)))
    orient = draw_orient(jax.random.fold_in(key_list[6], 71), 0)
    shifts = set_ends(jax.random.randint(key_list[3], (PARTICLES, NSHIFT, 2), -4, 5), jax.random.fold_in(key_list[3], 1), -4, 4).astype(jnp.int32)
    tilt = set_ends(jax.random.randint(key_list[4], (PARTICLES,), 0, TILTS), jax.random.fold_in(key_list[4], 1), 0, TILTS - 1).astype(jnp.int32)
    wedge = jnp.clip(0.1 + 0.9 * jax.random.uniform(key_list[5], (TILTS, BOX, BOX * BOX), jnp.float32) ** block_scale(key_list[5], (TILTS, BOX, BOX * BOX), ((1, 4),), -0.2, 0.2), 0.1, 1.0)
    return dict(particles=particles, refs=refs, orient=orient, shifts=shifts, tilt=tilt, wedge=wedge)


def dft_table(box):
    pixel = jnp.arange(box * box, dtype=jnp.int32)
    row_y = pixel // box
    row_x = pixel % box
    phase = (row_y[:, None] * row_y[None, :] + row_x[:, None] * row_x[None, :]) % box
    angle = phase.astype(jnp.float32) * (2.0 * math.pi / box)
    return jnp.concatenate([jnp.cos(angle), -jnp.sin(angle)], axis=1).astype(jnp.bfloat16)

def phases(shift_y, shift_x, box):
    freq = jnp.arange(box * box, dtype=jnp.int32)
    freq_y = freq // box
    freq_x = freq % box
    phase = (freq_y[None, :] * shift_y[:, None] + freq_x[None, :] * shift_x[:, None]) % box
    angle = phase.astype(jnp.float32) * (2.0 * math.pi / box)
    return (jnp.cos(angle), jnp.sin(angle))

def evaluate(cross, shifts, box):
    volume = box * box
    cross_re = cross[:, :volume]
    cross_im = cross[:, volume:]
    columns = []
    for cand in range(shifts.shape[1]):
        cosine, sine = phases(shifts[:, cand, 0], shifts[:, cand, 1], box)
        columns.append(lax.optimization_barrier(jnp.sum(cross_re * cosine - cross_im * sine, axis=1)) / volume)
    return jnp.stack(columns, axis=1)

def steer(weights, shifts, box):
    phi_re = jnp.zeros((shifts.shape[0], box * box), jnp.float32)
    phi_im = jnp.zeros((shifts.shape[0], box * box), jnp.float32)
    for cand in range(shifts.shape[1]):
        cosine, sine = phases(shifts[:, cand, 0], shifts[:, cand, 1], box)
        phi_re = phi_re + weights[:, cand:cand + 1] * cosine
        phi_im = phi_im + weights[:, cand:cand + 1] * sine
    return (phi_re, phi_im)

def reference(particles, refs, orient, shifts, tilt, wedge):
    total = particles.shape[0]
    box = particles.shape[1]
    volume = box * box
    table = dft_table(box).astype(jnp.float32)
    blocks = total // P_DEV

    def one_block(carry, index):
        acc_spec, acc_weight = carry
        start = (index * P_DEV).astype(jnp.int32)
        block = lax.dynamic_slice_in_dim(particles, start, P_DEV, 0)
        block_orient = lax.dynamic_slice_in_dim(orient, start, P_DEV, 0)
        block_shifts = lax.dynamic_slice_in_dim(shifts, start, P_DEV, 0)
        block_tilt = lax.dynamic_slice_in_dim(tilt, start, P_DEV, 0)
        flat = block.reshape(P_DEV * box, volume).astype(jnp.float32)
        spectrum = jnp.dot(flat, table, precision=lax.Precision.HIGHEST).reshape(P_DEV, box, 2 * volume)
        fetched = jnp.take(refs, block_orient, axis=0).astype(jnp.float32)
        spec_re = spectrum[:, :, :volume]
        spec_im = spectrum[:, :, volume:]
        ref_re = fetched[:, :, :volume]
        ref_im = fetched[:, :, volume:]
        cross = jnp.concatenate([lax.optimization_barrier(jnp.sum(spec_re * ref_re + spec_im * ref_im, axis=1)), lax.optimization_barrier(jnp.sum(spec_im * ref_re - spec_re * ref_im, axis=1))], axis=1)
        corr = evaluate(cross, block_shifts, box)
        score = corr / math.sqrt(box)
        square = score * score
        weights = square / (4.0 + lax.optimization_barrier(jnp.sum(square, axis=1, keepdims=True)))
        mass = lax.optimization_barrier(jnp.sum(weights, axis=1))
        phi_re, phi_im = steer(weights, block_shifts, box)
        wedge_rows = jnp.take(wedge, block_tilt, axis=0)
        part_re = wedge_rows * (phi_re[:, None, :] * spec_re - phi_im[:, None, :] * spec_im)
        part_im = wedge_rows * (phi_re[:, None, :] * spec_im + phi_im[:, None, :] * spec_re)
        contrib = jnp.concatenate([part_re, part_im], axis=2).astype(jnp.bfloat16)
        contrib = lax.optimization_barrier(contrib).astype(jnp.float32)
        acc_spec = acc_spec.at[block_orient].add(contrib)
        acc_weight = acc_weight.at[block_orient].add(wedge_rows * mass[:, None, None])
        return ((acc_spec, acc_weight), weights)
    start_spec = jnp.zeros(refs.shape, jnp.float32)
    start_weight = jnp.zeros((refs.shape[0], box, volume), jnp.float32)
    (acc_spec, acc_weight), weight_blocks = lax.scan(one_block, (start_spec, start_weight), jnp.arange(blocks, dtype=jnp.int32))
    shift_weights = weight_blocks.reshape(total, shifts.shape[1])
    denom = acc_weight + 1.0
    fresh = jnp.concatenate([acc_spec[:, :, :volume] / denom, acc_spec[:, :, volume:] / denom], axis=2)
    sumsq = lax.optimization_barrier(jnp.sum(fresh * fresh, axis=(1, 2)))
    rms = jnp.sqrt(sumsq / (box * volume))
    new_refs = fresh / jnp.maximum(rms, 1.0)[:, None, None]
    return (new_refs, shift_weights)
```

```python
import functools
import math

import jax
import jax.numpy as jnp
from jax import lax
from jax.experimental import pallas as pl
from jax.experimental.pallas import tpu as pltpu
from jax.sharding import PartitionSpec as P

BOX = 32
TILTS = 16
CHUNKS = 6
BINS = 128

HIGH = lax.Precision.HIGHEST
VMEM_SPEC = pl.BlockSpec(memory_space=pltpu.VMEM)
SMEM_SPEC = pl.BlockSpec(memory_space=pltpu.SMEM)
ANY_SPEC = pl.BlockSpec(memory_space=pl.ANY)


def dft_table(box):
    pixel = jnp.arange(box * box, dtype=jnp.int32)
    row_y = pixel // box
    row_x = pixel % box
    phase = (row_y[:, None] * row_y[None, :] + row_x[:, None] * row_x[None, :]) % box
    angle = phase.astype(jnp.float32) * (2.0 * math.pi / box)
    return jnp.concatenate([jnp.cos(angle), -jnp.sin(angle)], axis=1).astype(jnp.bfloat16)


def shift_table(box):
    bins = jnp.arange(BINS, dtype=jnp.int32)
    ty = bins // 9 - 4
    tx = bins % 9 - 4
    freq = jnp.arange(box * box, dtype=jnp.int32)
    phase = (ty[:, None] * (freq // box)[None, :] + tx[:, None] * (freq % box)[None, :]) % box
    angle = phase.astype(jnp.float32) * (2.0 * math.pi / box)
    return jnp.cos(angle), jnp.sin(angle)


def pick_kernel(holder_ref, rows_ref, out_ref):
    def step(s, carry):
        out_ref[s] = rows_ref[holder_ref[s]]
        return carry

    lax.fori_loop(0, out_ref.shape[0], step, 0, unroll=4)


def pick_rows(holder, rows):
    n = holder.shape[0]
    return pl.pallas_call(
        pick_kernel,
        out_shape=jax.ShapeDtypeStruct((n,) + rows.shape[1:], rows.dtype),
        in_specs=[SMEM_SPEC, VMEM_SPEC],
        out_specs=VMEM_SPEC,
        cost_estimate=pl.CostEstimate(flops=0, bytes_accessed=4 * 2**20, transcendentals=0),
    )(holder, rows)


def cross_kernel(local_ref, rows_ref, table_ref, eval_ref, refs_ref, spec_ref, every_ref, got, q, sem):
    n, planes, volume = rows_ref.shape

    def fetch(p, carry):
        pltpu.make_async_copy(refs_ref.at[local_ref[p]], got.at[p], sem).start()
        return carry

    lax.fori_loop(0, n, fetch, 0)
    flat = rows_ref[...].reshape(n * planes, volume)
    width = 256
    for at in range(0, volume, width):
        re = slice(at, at + width)
        im = slice(volume + at, volume + at + width)
        s_re = jnp.dot(flat, table_ref[:, re], preferred_element_type=jnp.float32)
        s_im = jnp.dot(flat, table_ref[:, im], preferred_element_type=jnp.float32)
        s_re = s_re.reshape(n, planes, width)
        s_im = s_im.reshape(n, planes, width)
        spec_ref[:, :, re] = s_re.astype(jnp.bfloat16)
        spec_ref[:, :, im] = s_im.astype(jnp.bfloat16)
        if at == 0:
            pltpu.make_async_copy(refs_ref.at[pl.ds(0, n)], got, sem).wait()
        r_re = got[:, :, re].astype(jnp.float32)
        r_im = got[:, :, im].astype(jnp.float32)
        q[:, re] = jnp.sum(s_re * r_re + s_im * r_im, axis=1)
        q[:, im] = jnp.sum(s_im * r_re - s_re * r_im, axis=1)
    every_ref[...] = jnp.dot(q[...], eval_ref[...], precision=HIGH, preferred_element_type=jnp.float32)


def cross(local, rows, table, evaluator, refs):
    n, planes, volume = rows.shape
    return pl.pallas_call(
        cross_kernel,
        out_shape=(
            jax.ShapeDtypeStruct((n, planes, 2 * volume), jnp.bfloat16),
            jax.ShapeDtypeStruct((n, BINS), jnp.float32),
        ),
        in_specs=[SMEM_SPEC, VMEM_SPEC, VMEM_SPEC, VMEM_SPEC, ANY_SPEC],
        out_specs=(VMEM_SPEC, VMEM_SPEC),
        scratch_shapes=[
            pltpu.VMEM((n, planes, 2 * volume), jnp.bfloat16),
            pltpu.VMEM((n, 2 * volume), jnp.float32),
            pltpu.SemaphoreType.DMA,
        ],
        compiler_params=pltpu.CompilerParams(vmem_limit_bytes=32 * 2**20),
        cost_estimate=pl.CostEstimate(
            flops=4 * n * planes * volume * volume, bytes_accessed=12 * 2**20, transcendentals=0
        ),
    )(local, rows, table, evaluator, refs)


def add_kernel(chunks, local_ref, tilt_ref, binned_ref, steer_ref, wedge_ref, *rest):
    specs = rest[:chunks]
    fresh_ref, sq_ref, weight, phi = rest[chunks:]
    owned, planes, two = fresh_ref.shape
    volume = two // 2
    n = specs[0].shape[0]
    phi[...] = jnp.dot(
        binned_ref[...], steer_ref[...], precision=HIGH, preferred_element_type=jnp.float32
    )

    def clear(o, carry):
        fresh_ref[o] = jnp.zeros((planes, two), jnp.float32)
        weight[o] = jnp.zeros((planes, volume), jnp.float32)
        return carry

    lax.fori_loop(0, owned, clear, 0, unroll=2)
    for c in range(chunks):
        spec_ref = specs[c]

        def add(j, carry, c=c, spec_ref=spec_ref):
            p = c * n + j
            o = local_ref[p]

            @pl.when(o >= 0)
            def _():
                wed = wedge_ref[tilt_ref[p]]
                row = pl.ds(p, 1)
                p_re = phi[row, :volume] * wed
                p_im = phi[row, volume:two] * wed
                s_re = spec_ref[j, :, :volume].astype(jnp.float32)
                s_im = spec_ref[j, :, volume:].astype(jnp.float32)
                fresh_ref[o, :, :volume] += p_re * s_re - p_im * s_im
                fresh_ref[o, :, volume:] += p_re * s_im + p_im * s_re
                weight[o] += phi[row, two:] * wed

            return carry

        lax.fori_loop(0, n, add, 0)

    def finish(o, carry):
        inv = 1.0 / (weight[o] + 1.0)
        a_re = fresh_ref[o, :, :volume] * inv
        a_im = fresh_ref[o, :, volume:] * inv
        fresh_ref[o, :, :volume] = a_re
        fresh_ref[o, :, volume:] = a_im
        total = a_re * a_re + a_im * a_im
        part = total[:, :128]
        for at in range(128, volume, 128):
            part = part + total[:, at : at + 128]
        sq_ref[o] = part
        return carry

    lax.fori_loop(0, owned, finish, 0, unroll=2)


def accumulate(local, tilt, binned, steerer, wedge, specs, owned):
    n, planes, two = specs[0].shape
    volume = two // 2
    chunks = len(specs)
    return pl.pallas_call(
        functools.partial(add_kernel, chunks),
        out_shape=(
            jax.ShapeDtypeStruct((owned, planes, two), jnp.float32),
            jax.ShapeDtypeStruct((owned, planes, 128), jnp.float32),
        ),
        in_specs=[SMEM_SPEC, SMEM_SPEC] + [VMEM_SPEC] * (3 + chunks),
        out_specs=(VMEM_SPEC, VMEM_SPEC),
        scratch_shapes=[
            pltpu.VMEM((owned, planes, volume), jnp.float32),
            pltpu.VMEM((chunks * n, 3 * volume), jnp.float32),
        ],
        compiler_params=pltpu.CompilerParams(vmem_limit_bytes=56 * 2**20),
        cost_estimate=pl.CostEstimate(
            flops=20 * n * chunks * planes * volume, bytes_accessed=64 * 2**20, transcendentals=0
        ),
    )(local, tilt, binned, steerer, wedge, *specs)


def shards(particles, refs, orient, shifts, tilt, wedge):
    count, planes, volume = particles.shape
    owned = refs.shape[0]
    ncand = shifts.shape[1]
    peers = lax.axis_size("dom")
    capacity = 2 * count // peers
    slots_all = peers * capacity
    each = capacity // CHUNKS
    rows_chunk = peers * each

    owner = orient // owned
    index = jnp.arange(count, dtype=jnp.int32)
    same = (owner[:, None] == owner[None, :]) & (index[None, :] < index[:, None])
    rank = jnp.sum(same.astype(jnp.int32), axis=1)
    slot = (rank // each) * rows_chunk + owner * each + rank % each
    slot_hot = slot[None, :] == jnp.arange(slots_all, dtype=jnp.int32)[:, None]
    holder = jnp.sum(jnp.where(slot_hot, index[None, :], 0), axis=1)
    bins = (shifts[:, :, 0] + 4) * 9 + (shifts[:, :, 1] + 4)
    meta = jnp.concatenate([(orient % owned)[:, None] + 1, tilt[:, None], bins], axis=1)
    sent_meta = jnp.dot(
        slot_hot.astype(jnp.float32), meta.astype(jnp.float32), precision=HIGH
    )
    width = ncand + 2
    sent_meta = sent_meta.reshape(CHUNKS, peers, each, width).transpose(1, 0, 2, 3)
    in_meta = lax.all_to_all(
        sent_meta.reshape(peers, CHUNKS * each * width), "dom", split_axis=0, concat_axis=0, tiled=True
    )
    in_meta = in_meta.reshape(peers, CHUNKS, each, width).transpose(1, 0, 2, 3)
    in_meta = jnp.round(in_meta.reshape(slots_all, width)).astype(jnp.int32)
    local = in_meta[:, 0] - 1
    work_tilt = in_meta[:, 1]
    work_bins = in_meta[:, 2:]
    safe = jnp.maximum(local, 0)

    table = dft_table(BOX)
    cosine, sine = shift_table(BOX)
    evaluator = jnp.concatenate([cosine.T, -sine.T], axis=0) / volume
    steerer = jnp.concatenate([cosine, sine, jnp.ones_like(cosine)], axis=1)

    specs = []
    everys = []
    for c in range(CHUNKS):
        part = slice(c * rows_chunk, (c + 1) * rows_chunk)
        out_rows = pick_rows(holder[part], particles)
        in_rows = lax.all_to_all(
            out_rows.reshape(peers, each, planes, volume), "dom", split_axis=0, concat_axis=0, tiled=True
        )
        spec, every = cross(
            safe[part], in_rows.reshape(rows_chunk, planes, volume), table, evaluator, refs
        )
        specs.append(spec)
        everys.append(every)
    every = jnp.concatenate(everys, axis=0)
    hot = (work_bins[:, :, None] == jnp.arange(BINS, dtype=jnp.int32)[None, None, :]).astype(
        jnp.float32
    )
    corr = jnp.sum(hot * every[:, None, :], axis=2)
    corr = jnp.sum(
        lax.all_gather(corr.T.reshape(-1, 128), "slab", axis=0, tiled=False), axis=0
    ).reshape(ncand, slots_all).T
    score = corr / math.sqrt(BOX)
    square = score * score
    weights = square / (4.0 + jnp.sum(square, axis=1, keepdims=True))
    binned = jnp.sum(hot * weights[:, :, None], axis=1)
    fresh, sq = accumulate(local, work_tilt, binned, steerer, wedge, specs, owned)

    back = lax.all_to_all(
        weights.reshape(CHUNKS, peers, each * ncand).transpose(1, 0, 2).reshape(peers, -1),
        "dom",
        split_axis=0,
        concat_axis=0,
        tiled=True,
    )
    back = back.reshape(peers, CHUNKS, each, ncand).transpose(1, 0, 2, 3).reshape(slots_all, ncand)
    shift_weights = jnp.dot(slot_hot.T.astype(jnp.float32), back, precision=HIGH)

    sums = jnp.sum(sq, axis=(1, 2))
    sumsq = jnp.sum(lax.all_gather(sums, "slab", axis=0, tiled=False), axis=0)
    rms = jnp.sqrt(sumsq / (BOX * volume))
    new_refs = fresh / jnp.maximum(rms, 1.0)[:, None, None]
    return (new_refs, shift_weights)


def solution(mesh):
    placed = (
        P("dom", "slab", None),
        P("dom", "slab", None),
        P("dom"),
        P("dom", None, None),
        P("dom"),
        P(None, "slab", None),
    )
    return jax.shard_map(
        shards,
        mesh=mesh,
        in_specs=placed,
        out_specs=(P("dom", "slab", None), P("dom", None)),
        check_vma=False,
    )
```

```python
import functools
import math

import jax
import jax.numpy as jnp
from jax import lax
from jax.experimental import pallas as pl
from jax.experimental.pallas import tpu as pltpu
from jax.sharding import PartitionSpec as P

BOX = 32
CHUNKS = 6
BINS = 128

MESH = pl.DeviceIdType.MESH
HIGH = lax.Precision.HIGHEST
VMEM_SPEC = pl.BlockSpec(memory_space=pltpu.VMEM)
SMEM_SPEC = pl.BlockSpec(memory_space=pltpu.SMEM)
ANY_SPEC = pl.BlockSpec(memory_space=pl.ANY)


def phase_rows(rows, cols, row_at, col_at, box):
    pixel = lax.broadcasted_iota(jnp.int32, (rows, cols), 0) + row_at
    freq = lax.broadcasted_iota(jnp.int32, (rows, cols), 1) + col_at
    phase = ((pixel // box) * (freq // box) + (pixel % box) * (freq % box)) % box
    return phase.astype(jnp.float32) * (2.0 * math.pi / box)


def shift_rows(cols, box):
    bins = lax.broadcasted_iota(jnp.int32, (BINS, cols), 0)
    freq = lax.broadcasted_iota(jnp.int32, (BINS, cols), 1)
    phase = ((bins // 9 - 4) * (freq // box) + (bins % 9 - 4) * (freq % box) + 32 * box) % box
    return phase.astype(jnp.float32) * (2.0 * math.pi / box)


def pick_kernel(holder_ref, rows_ref, out_ref):
    def step(s, carry):
        out_ref[s] = rows_ref[holder_ref[s]]
        return carry

    lax.fori_loop(0, out_ref.shape[0], step, 0, unroll=4)


def pick_rows(holder, rows):
    n = holder.shape[0]
    return pl.pallas_call(
        pick_kernel,
        out_shape=jax.ShapeDtypeStruct((n,) + rows.shape[1:], rows.dtype),
        in_specs=[SMEM_SPEC, VMEM_SPEC],
        out_specs=VMEM_SPEC,
        cost_estimate=pl.CostEstimate(flops=0, bytes_accessed=4 * 2**20, transcendentals=0),
    )(holder, rows)


def exchange_kernel(
    peers, out_ref, meta_ref, refs_ref,
    spec_ref, every_ref, in_meta_ref, steer_ref,
    rows, table, got, q, stage, index_ref,
    send, recv, own_sem, meta_send, meta_recv, local_sem, spec_sem,
):
    chunks, _, each, planes, volume = out_ref.shape
    n = peers * each
    me = lax.axis_index("dom")
    barrier = pltpu.get_barrier_semaphore()
    for k in range(1, peers):
        pl.semaphore_signal(
            barrier, inc=1, device_id={"dom": lax.rem(me + k, peers)}, device_id_type=MESH
        )
    pl.semaphore_wait(barrier, peers - 1)

    def meta_copy(k):
        to = lax.rem(me + k, peers)
        return pltpu.make_async_remote_copy(
            src_ref=meta_ref.at[to], dst_ref=in_meta_ref.at[me],
            send_sem=meta_send.at[k], recv_sem=meta_recv.at[k],
            device_id={"dom": to}, device_id_type=MESH,
        )

    def row_copy(c, k):
        to = lax.rem(me + k, peers)
        return pltpu.make_async_remote_copy(
            src_ref=out_ref.at[c, to], dst_ref=rows.at[c, me],
            send_sem=send.at[c, k], recv_sem=recv.at[c, k],
            device_id={"dom": to}, device_id_type=MESH,
        )

    def start_meta(k, carry):
        meta_copy(k).start()
        return carry

    lax.fori_loop(1, peers, start_meta, 0)

    def start_rows(i, carry):
        row_copy(i // (peers - 1), i % (peers - 1) + 1).start()
        return carry

    lax.fori_loop(0, chunks * (peers - 1), start_rows, 0)
    own_meta = pltpu.make_async_copy(meta_ref.at[me], in_meta_ref.at[me], local_sem)
    own_meta.start()
    own = pltpu.make_async_copy(out_ref.at[:, me], rows.at[:, me], own_sem)
    own.start()

    tile = 128

    def fill(i, carry):
        at = pl.multiple_of(i * tile, tile)
        for j in range(0, volume, tile):
            angle = phase_rows(tile, tile, at, j, BOX)
            table[pl.ds(at, tile), j : j + tile] = jnp.cos(angle).astype(jnp.bfloat16)
            table[pl.ds(at, tile), volume + j : volume + j + tile] = (-jnp.sin(angle)).astype(
                jnp.bfloat16
            )
        return carry

    lax.fori_loop(0, volume // tile, fill, 0)
    angle = shift_rows(volume, BOX)
    steer_ref[:, :volume] = jnp.cos(angle)
    steer_ref[:, volume:] = jnp.sin(angle)

    own_meta.wait()

    def wait_meta(k, carry):
        meta_copy(k).wait()
        return carry

    lax.fori_loop(1, peers, wait_meta, 0)
    to_smem = pltpu.make_async_copy(in_meta_ref, index_ref, local_sem)
    to_smem.start()
    to_smem.wait()
    own.wait()

    def spec_copy(c):
        slot = c % 2
        return pltpu.make_async_copy(
            stage.at[slot], spec_ref.at[pl.ds(c * n, n)], spec_sem.at[slot]
        )

    def one_chunk(c, carry):
        def fetch(i, carry):
            o = index_ref[i // each, 0, c * each + i % each]
            got[i] = refs_ref[o]
            return carry

        lax.fori_loop(0, n, fetch, 0)

        def wait_rows(k, carry):
            row_copy(c, k).wait()
            return carry

        lax.fori_loop(1, peers, wait_rows, 0)

        @pl.when(c >= 2)
        def _():
            spec_copy(c - 2).wait()

        flat = rows[c].reshape(n * planes, volume)
        slot = c % 2
        width = 256
        for at in range(0, volume, width):
            re = slice(at, at + width)
            im = slice(volume + at, volume + at + width)
            s_re = jnp.dot(flat, table[:, re], preferred_element_type=jnp.float32)
            s_im = jnp.dot(flat, table[:, im], preferred_element_type=jnp.float32)
            s_re = s_re.reshape(n, planes, width)
            s_im = s_im.reshape(n, planes, width)
            stage[slot, :, :, re] = s_re.astype(jnp.bfloat16)
            stage[slot, :, :, im] = s_im.astype(jnp.bfloat16)
            r_re = got[:, :, re].astype(jnp.float32)
            r_im = got[:, :, im].astype(jnp.float32)
            q[:, re] = jnp.sum(s_re * r_re + s_im * r_im, axis=1)
            q[:, im] = jnp.sum(s_im * r_re - s_re * r_im, axis=1)
        nt = (((1,), (1,)), ((), ()))
        every_ref[pl.ds(c * n, n), :] = (
            lax.dot_general(
                q[:, :volume], steer_ref[:, :volume], nt, precision=HIGH,
                preferred_element_type=jnp.float32,
            )
            - lax.dot_general(
                q[:, volume:], steer_ref[:, volume:], nt, precision=HIGH,
                preferred_element_type=jnp.float32,
            )
        ) * (1.0 / volume)
        spec_copy(c).start()
        return carry

    lax.fori_loop(0, chunks, one_chunk, 0)
    for c in range(max(chunks - 2, 0), chunks):
        spec_copy(c).wait()


def exchange(out_rows, sent_meta, refs):
    chunks, peers, each, planes, volume = out_rows.shape
    n = peers * each
    owned = refs.shape[0]
    return pl.pallas_call(
        functools.partial(exchange_kernel, peers),
        out_shape=(
            jax.ShapeDtypeStruct((chunks * n, planes, 2 * volume), jnp.bfloat16),
            jax.ShapeDtypeStruct((chunks * n, BINS), jnp.float32),
            jax.ShapeDtypeStruct(sent_meta.shape, jnp.int32),
            jax.ShapeDtypeStruct((BINS, 2 * volume), jnp.float32),
        ),
        in_specs=[ANY_SPEC, VMEM_SPEC, VMEM_SPEC],
        out_specs=(ANY_SPEC, VMEM_SPEC, VMEM_SPEC, VMEM_SPEC),
        scratch_shapes=[
            pltpu.VMEM((chunks, peers, each, planes, volume), jnp.bfloat16),
            pltpu.VMEM((volume, 2 * volume), jnp.bfloat16),
            pltpu.VMEM((n, planes, 2 * volume), jnp.bfloat16),
            pltpu.VMEM((n, 2 * volume), jnp.float32),
            pltpu.VMEM((2, n, planes, 2 * volume), jnp.bfloat16),
            pltpu.SMEM(sent_meta.shape, jnp.int32),
            pltpu.SemaphoreType.DMA((chunks, peers)),
            pltpu.SemaphoreType.DMA((chunks, peers)),
            pltpu.SemaphoreType.DMA,
            pltpu.SemaphoreType.DMA((peers,)),
            pltpu.SemaphoreType.DMA((peers,)),
            pltpu.SemaphoreType.DMA,
            pltpu.SemaphoreType.DMA((2,)),
        ],
        compiler_params=pltpu.CompilerParams(
            collective_id=0, has_side_effects=True, vmem_limit_bytes=48 * 2**20
        ),
    )(out_rows, sent_meta, refs)


def add_kernel(
    local_ref, tilt_ref, binned_ref, mass_ref, steer_ref, wedge_ref, spec_ref, fresh_ref, sq_ref,
    weight, phi, spec, sems
):
    owned, planes, two = fresh_ref.shape
    volume = two // 2
    chunks, n = spec.shape[:2]

    def load(c):
        return pltpu.make_async_copy(spec_ref.at[pl.ds(c * n, n)], spec.at[c], sems.at[c])

    for c in range(chunks):
        load(c).start()
    phi[...] = jnp.dot(
        binned_ref[...], steer_ref[...], precision=HIGH, preferred_element_type=jnp.float32
    )

    def clear(o, carry):
        fresh_ref[o] = jnp.zeros((planes, two), jnp.float32)
        weight[o] = jnp.zeros((planes, volume), jnp.float32)
        return carry

    lax.fori_loop(0, owned, clear, 0, unroll=2)
    for c in range(chunks):
        load(c).wait()

        def add(j, carry, c=c):
            p = c * n + j
            o = local_ref[p]

            @pl.when(o >= 0)
            def _():
                wed = wedge_ref[tilt_ref[p]]
                row = pl.ds(p, 1)
                p_re = phi[row, :volume] * wed
                p_im = phi[row, volume:two] * wed
                s_re = spec[c, j, :, :volume].astype(jnp.float32)
                s_im = spec[c, j, :, volume:].astype(jnp.float32)
                fresh_ref[o, :, :volume] += p_re * s_re - p_im * s_im
                fresh_ref[o, :, volume:] += p_re * s_im + p_im * s_re
                weight[o] += mass_ref[p] * wed

            return carry

        lax.fori_loop(0, n, add, 0)

    def finish(o, carry):
        inv = 1.0 / (weight[o] + 1.0)
        a_re = fresh_ref[o, :, :volume] * inv
        a_im = fresh_ref[o, :, volume:] * inv
        fresh_ref[o, :, :volume] = a_re
        fresh_ref[o, :, volume:] = a_im
        total = a_re * a_re + a_im * a_im
        part = total[:, :128]
        for at in range(128, volume, 128):
            part = part + total[:, at : at + 128]
        sq_ref[o] = part
        return carry

    lax.fori_loop(0, owned, finish, 0, unroll=2)


def accumulate(local, tilt, binned, mass, steerer, wedge, spec, owned):
    slots, planes, two = spec.shape
    volume = two // 2
    n = slots // CHUNKS
    return pl.pallas_call(
        add_kernel,
        out_shape=(
            jax.ShapeDtypeStruct((owned, planes, two), jnp.float32),
            jax.ShapeDtypeStruct((owned, planes, 128), jnp.float32),
        ),
        in_specs=[SMEM_SPEC, SMEM_SPEC, VMEM_SPEC, SMEM_SPEC, VMEM_SPEC, VMEM_SPEC, ANY_SPEC],
        out_specs=(VMEM_SPEC, VMEM_SPEC),
        scratch_shapes=[
            pltpu.VMEM((owned, planes, volume), jnp.float32),
            pltpu.VMEM((slots, two), jnp.float32),
            pltpu.VMEM((CHUNKS, n, planes, two), jnp.bfloat16),
            pltpu.SemaphoreType.DMA((CHUNKS,)),
        ],
        compiler_params=pltpu.CompilerParams(vmem_limit_bytes=56 * 2**20),
        cost_estimate=pl.CostEstimate(
            flops=20 * slots * planes * volume, bytes_accessed=64 * 2**20, transcendentals=0
        ),
    )(local, tilt, binned, mass, steerer, wedge, spec)


def shards(particles, refs, orient, shifts, tilt, wedge):
    count, planes, volume = particles.shape
    owned = refs.shape[0]
    ncand = shifts.shape[1]
    peers = lax.axis_size("dom")
    capacity = 2 * count // peers
    slots_all = peers * capacity
    each = capacity // CHUNKS
    rows_chunk = peers * each

    owner = orient // owned
    index = jnp.arange(count, dtype=jnp.int32)
    same = (owner[:, None] == owner[None, :]) & (index[None, :] < index[:, None])
    rank = jnp.sum(same.astype(jnp.int32), axis=1)
    slot = (rank // each) * rows_chunk + owner * each + rank % each
    slot_hot = slot[None, :] == jnp.arange(slots_all, dtype=jnp.int32)[:, None]
    holder = jnp.sum(jnp.where(slot_hot, index[None, :], 0), axis=1)
    bins = (shifts[:, :, 0] + 4) * 9 + (shifts[:, :, 1] + 4)
    fields = [orient % owned, jnp.ones_like(orient), tilt] + [bins[:, k] for k in range(ncand)]
    height = -(-len(fields) // 8) * 8
    lanes = -(-capacity // 128) * 128
    meta = jnp.stack(fields + [jnp.zeros_like(orient)] * (height - len(fields)), axis=0)
    place_hot = rank[:, None] == jnp.arange(lanes, dtype=jnp.int32)[None, :]
    owner_hot = owner[None, :] == jnp.arange(peers, dtype=jnp.int32)[:, None]
    spread = (owner_hot[:, None, :] * meta[None, :, :]).astype(jnp.float32)
    sent_meta = jnp.dot(
        spread.reshape(peers * height, count), place_hot.astype(jnp.float32), precision=HIGH
    )
    sent_meta = jnp.round(sent_meta).astype(jnp.int32).reshape(peers, height, lanes)
    out_rows = pick_rows(holder, particles).reshape(CHUNKS, peers, each, planes, volume)
    spec, every, in_meta, steerer = exchange(out_rows, sent_meta, refs)
    in_meta = in_meta[:, : 3 + ncand, :capacity].reshape(peers, 3 + ncand, CHUNKS, each)
    in_meta = in_meta.transpose(1, 2, 0, 3).reshape(3 + ncand, slots_all)
    local = jnp.where(in_meta[1] > 0, in_meta[0], -1)
    work_tilt = in_meta[2]
    work_bins = in_meta[3:].T
    hot = (work_bins[:, :, None] == jnp.arange(BINS, dtype=jnp.int32)[None, None, :]).astype(
        jnp.float32
    )
    corr = jnp.sum(hot * every[:, None, :], axis=2)
    corr = jnp.sum(
        lax.all_gather(corr.T.reshape(-1, 128), "slab", axis=0, tiled=False), axis=0
    ).reshape(ncand, slots_all).T
    score = corr / math.sqrt(BOX)
    square = score * score
    weights = square / (4.0 + jnp.sum(square, axis=1, keepdims=True))
    binned = jnp.sum(hot * weights[:, :, None], axis=1)
    mass = jnp.sum(weights, axis=1)
    fresh, sq = accumulate(local, work_tilt, binned, mass, steerer, wedge, spec, owned)

    back = lax.all_to_all(
        weights.reshape(CHUNKS, peers, each * ncand).transpose(1, 0, 2).reshape(peers, -1),
        "dom",
        split_axis=0,
        concat_axis=0,
        tiled=True,
    )
    back = back.reshape(peers, CHUNKS, each, ncand).transpose(1, 0, 2, 3).reshape(slots_all, ncand)
    shift_weights = jnp.dot(slot_hot.T.astype(jnp.float32), back, precision=HIGH)

    sums = jnp.sum(sq, axis=(1, 2))
    sumsq = jnp.sum(lax.all_gather(sums, "slab", axis=0, tiled=False), axis=0)
    rms = jnp.sqrt(sumsq / (BOX * volume))
    new_refs = fresh / jnp.maximum(rms, 1.0)[:, None, None]
    return (new_refs, shift_weights)


def solution(mesh):
    placed = (
        P("dom", "slab", None),
        P("dom", "slab", None),
        P("dom"),
        P("dom", None, None),
        P("dom"),
        P(None, "slab", None),
    )
    return jax.shard_map(
        shards,
        mesh=mesh,
        in_specs=placed,
        out_specs=(P("dom", "slab", None), P("dom", None)),
        check_vma=False,
    )
```
